32 devices in a mesh: shard: 8 (over y, x, core), replica: 4 (over z).
Axes of the slice: x: 2, y: 2, z: 4, core: 2. Of those that a mesh axis runs over, the one named last changes fastest.
Arguments:
- custkey: int32 [262144], P(('shard', 'replica')), may hold values from 0 to 8191
- quarter: int32 [262144], P(('shard', 'replica')), may hold values from 0 to 27
- revenue: float32 [262144], P(('shard', 'replica')), may hold values from -6 to 6
- segment: int32 [8192], P('shard'), may hold values from 0 to 4
- rate: bfloat16 [8192], P('shard'), may hold values from 0.25 to 4
Outputs:
- cube: float32 [5, 28], replicated
The draws below stay inside these ranges and needn't reach their ends.
All inputs are finite; a program needn't handle non-finite values.
Results may differ from the reference program's by a relative error of at most 0.0003.
Values may be sent and summed in bfloat16 or wider, within the bound.
No kernel may reach another device: no remote copies, remote signals or barrier semaphores. Data moves between devices by JAX's collectives and lax.ppermute only.
A program may use at most 64 MiB of HBM per device.

```python
import math
import jax
import jax.numpy as jnp

SEGMENTS = 5
QUARTERS = 28
FACT_ROWS = 262144
CUSTOMERS = 8192


def set_ends(entries, stream_key, smallest, largest):
    longest = entries.shape.index(max(entries.shape))
    spots = []
    for shift in (0, 1):
        where = [jax.random.randint(jax.random.fold_in(stream_key, axis), (), 0, length) for axis, length in enumerate(entries.shape)]
        where[longest] = (where[longest] + shift) % entries.shape[longest]
        spots.append(tuple(where))
    return entries.at[spots[0]].set(smallest).at[spots[1]].set(largest)


def steps_of(rng, dims, split, low, high):
    level, own = 1.0, jax.random.fold_in(rng, 6)
    for axis_at, parts in split:
        draws = jnp.exp(jax.random.uniform(jax.random.fold_in(own, axis_at), (parts,), jnp.float32, low / len(split), high / len(split)))
        level = level * jnp.repeat(draws, dims[axis_at] // parts).reshape([-1 if axis == axis_at else 1 for axis in range(len(dims))])
    return level


def normal_values(key, shape, scale, bound, pieces=(), kind=jnp.bfloat16):
    drawn = jax.random.normal(key, shape, jnp.float32) * scale
    if len(pieces) > 0:
        drawn = steps_of(key, shape, pieces, -0.22, 0.18) * drawn
    return jnp.clip(drawn, min=-bound, max=bound).astype(kind)


def setup_inputs(seed: int = 0) -> dict:
    splits = jax.random.split(jax.random.key(seed), 6)
    custkey = set_ends(jax.random.randint(splits[0], (FACT_ROWS,), 0, CUSTOMERS), jax.random.fold_in(splits[0], 1), 0, CUSTOMERS - 1).astype(jnp.int32)
    quarter = set_ends(jax.random.randint(splits[1], (FACT_ROWS,), 0, QUARTERS), jax.random.fold_in(splits[1], 1), 0, QUARTERS - 1).astype(jnp.int32)
    revenue = normal_values(splits[2], (FACT_ROWS,), 1.0, 6.0, ((0, 32),), jnp.float32)
    segment = set_ends(jax.random.randint(splits[3], (CUSTOMERS,), 0, SEGMENTS), jax.random.fold_in(splits[3], 1), 0, SEGMENTS - 1).astype(jnp.int32)
    rate = jnp.clip(jnp.exp(math.log(4.0) - 2.7725887 * jax.random.uniform(splits[4], (CUSTOMERS,), jnp.float32) ** steps_of(splits[4], (CUSTOMERS,), ((0, 8),), -0.2, 0.2)), 0.25, 4.0).astype(jnp.bfloat16)
    return {"custkey": custkey, "quarter": quarter, "revenue": revenue, "segment": segment, "rate": rate}


def reference(custkey, quarter, revenue, segment, rate):
    seg = segment[custkey]
    factor = rate[custkey].astype(jnp.float32)
    weight = revenue * factor
    cell = (seg * QUARTERS + quarter).astype(jnp.int32)
    cube = jax.ops.segment_sum(weight, cell, num_segments=SEGMENTS * QUARTERS)
    return cube.reshape(SEGMENTS, QUARTERS)
```

```python
import jax
import jax.numpy as jnp
from jax import lax
from jax.experimental import pallas as pl
from jax.experimental.pallas import tpu as pltpu
from jax.sharding import PartitionSpec as P

SEGMENTS = 5
QUARTERS = 28
SUBLANES = 8
LANES = 128
STEP = 8.0


def sublane_sums(parts):
    row = lax.broadcasted_iota(jnp.int32, (SUBLANES, LANES), 0)

    def merge(a, b, width, bit):
        keep = (row & bit) == 0
        if b is None:
            return a + pltpu.roll(a, width, 0)
        return jnp.where(keep, a, b) + pltpu.roll(jnp.where(keep, b, a), width, 0)

    a0, a1, a2, a3, a4 = parts
    a0 = merge(a0, a4, 4, 4)
    a1, a2, a3 = (merge(a, None, 4, 4) for a in (a1, a2, a3))
    def fold(a, b, width):
        keep = (row & width) == 0
        up = jnp.where(keep, pltpu.roll(a, SUBLANES - width, 0), pltpu.roll(b, width, 0))
        return jnp.where(keep, a, b) + up

    a0, a1 = fold(a0, a2, 2), fold(a1, a3, 2)
    return fold(a0, a1, 1)


def cube_kernel(table_ref, custkey_ref, quarter_ref, revenue_ref, out_ref):
    rows = table_ref.shape[0]
    chunks = custkey_ref.shape[0] // SUBLANES
    at = [pl.ds(c * SUBLANES, SUBLANES) for c in range(chunks)]
    keys = [custkey_ref[a, :] for a in at]
    high = [k // LANES for k in keys]
    low = [k % LANES for k in keys]

    def look(step, found):
        base = pl.multiple_of(step * SUBLANES, SUBLANES)
        found = list(found)
        for r in range(SUBLANES):
            line = jnp.broadcast_to(table_ref[pl.ds(base + r, 1), :], (SUBLANES, LANES))
            for c in range(chunks):
                got = jnp.take_along_axis(line, low[c], axis=1)
                found[c] = jnp.where(high[c] == base + r, got, found[c])
        return tuple(found)

    zero = jnp.zeros((SUBLANES, LANES), jnp.float32)
    found = lax.fori_loop(0, rows // SUBLANES, look, (zero,) * chunks)
    weights = []
    for c in range(chunks):
        segment = jnp.floor(found[c] * (1.0 / STEP))
        weight = revenue_ref[at[c], :] * (found[c] - segment * STEP)
        weights.append([jnp.where(segment == s, weight, 0.0) for s in range(SEGMENTS)])
    quarters = [quarter_ref[a, :] for a in at]
    lane = lax.broadcasted_iota(jnp.int32, (SUBLANES, LANES), 1)
    cube = zero
    for q in range(QUARTERS):
        inside = [x == q for x in quarters]
        parts = []
        for s in range(SEGMENTS):
            total = zero
            for c in range(chunks):
                total = total + jnp.where(inside[c], weights[c][s], 0.0)
            parts.append(total)
        sums = jnp.sum(sublane_sums(parts), axis=1, keepdims=True)
        cube = jnp.where(lane == q, sums, cube)
    for d in range(out_ref.shape[0]):
        out_ref[d] = cube


def solution(mesh):
    shards = mesh.shape["shard"]
    everyone = shards * mesh.shape["replica"]

    def per_device(custkey, quarter, revenue, segment, rate):
        mine = segment.astype(jnp.float32) * STEP + rate.astype(jnp.float32)
        mine = mine.reshape(-1, LANES)
        table = lax.all_to_all(
            jnp.broadcast_to(mine[None], (shards, *mine.shape)), "shard", 0, 0
        )
        partial_cubes = pl.pallas_call(
            cube_kernel,
            out_shape=jax.ShapeDtypeStruct((everyone, SUBLANES, LANES), jnp.float32),
        )(
            table.reshape(-1, LANES),
            custkey.reshape(-1, LANES),
            quarter.reshape(-1, LANES),
            revenue.reshape(-1, LANES),
        )
        cubes = lax.all_to_all(partial_cubes, ("shard", "replica"), 0, 0)
        return jnp.sum(cubes, axis=0)[:SEGMENTS, :QUARTERS]

    return jax.shard_map(
        per_device,
        mesh=mesh,
        in_specs=(
            P(("shard", "replica")),
            P(("shard", "replica")),
            P(("shard", "replica")),
            P("shard"),
            P("shard"),
        ),
        out_specs=P(),
        check_vma=False,
    )
```

```python
import jax
import jax.numpy as jnp
from jax import lax
from jax.experimental import pallas as pl
from jax.experimental.pallas import tpu as pltpu
from jax.sharding import PartitionSpec as P

SEGMENTS = 5
QUARTERS = 28
SUBLANES = 8
LANES = 128
STEP = 8.0


def sublane_sums(parts):
    row = lax.broadcasted_iota(jnp.int32, (SUBLANES, LANES), 0)

    def merge(a, b, width, bit):
        keep = (row & bit) == 0
        if b is None:
            return a + pltpu.roll(a, width, 0)
        return jnp.where(keep, a, b) + pltpu.roll(jnp.where(keep, b, a), width, 0)

    a0, a1, a2, a3, a4 = parts
    a0 = merge(a0, a4, 4, 4)
    a1, a2, a3 = (merge(a, None, 4, 4) for a in (a1, a2, a3))
    def fold(a, b, width):
        keep = (row & width) == 0
        up = jnp.where(keep, pltpu.roll(a, SUBLANES - width, 0), pltpu.roll(b, width, 0))
        return jnp.where(keep, a, b) + up

    a0, a1 = fold(a0, a2, 2), fold(a1, a3, 2)
    return fold(a0, a1, 1)


def cube_kernel(table_ref, custkey_ref, quarter_ref, revenue_ref, out_ref):
    rows = table_ref.shape[0]
    chunks = custkey_ref.shape[0] // SUBLANES
    at = [pl.ds(c * SUBLANES, SUBLANES) for c in range(chunks)]
    keys = [custkey_ref[a, :] for a in at]
    high = [k // LANES for k in keys]
    low = [k % LANES for k in keys]

    def look(step, found):
        base = pl.multiple_of(step * SUBLANES, SUBLANES)
        found = list(found)
        for r in range(SUBLANES):
            line = jnp.broadcast_to(table_ref[pl.ds(base + r, 1), :], (SUBLANES, LANES))
            for c in range(chunks):
                got = jnp.take_along_axis(line, low[c], axis=1)
                found[c] = jnp.where(high[c] == base + r, got, found[c])
        return tuple(found)

    zero = jnp.zeros((SUBLANES, LANES), jnp.float32)
    found = lax.fori_loop(0, rows // SUBLANES, look, (zero,) * chunks)
    weights = []
    for c in range(chunks):
        segment = jnp.floor(found[c] * (1.0 / STEP))
        weight = revenue_ref[at[c], :] * (found[c] - segment * STEP)
        weights.append([jnp.where(segment == s, weight, 0.0) for s in range(SEGMENTS)])
    quarters = [quarter_ref[a, :] for a in at]
    lane = lax.broadcasted_iota(jnp.int32, (SUBLANES, LANES), 1)
    cube = zero
    for q in range(QUARTERS):
        inside = [x == q for x in quarters]
        parts = []
        for s in range(SEGMENTS):
            total = zero
            for c in range(chunks):
                total = total + jnp.where(inside[c], weights[c][s], 0.0)
            parts.append(total)
        sums = jnp.sum(sublane_sums(parts), axis=1, keepdims=True)
        cube = jnp.where(lane == q, sums, cube)
    for d in range(out_ref.shape[0]):
        out_ref[d] = cube


def solution(mesh):
    shards = mesh.shape["shard"]
    everyone = shards * mesh.shape["replica"]

    def per_device(custkey, quarter, revenue, segment, rate):
        mine = segment.astype(jnp.float32) * STEP + rate.astype(jnp.float32)
        mine = mine.reshape(-1, LANES)
        table = lax.all_to_all(
            jnp.broadcast_to(mine[None], (shards, *mine.shape)), "shard", 0, 0
        )
        partial_cubes = pl.pallas_call(
            cube_kernel,
            out_shape=jax.ShapeDtypeStruct((everyone, SUBLANES, LANES), jnp.float32),
            compiler_params=pltpu.CompilerParams(vmem_limit_bytes=4 * 2**20),
        )(
            table.reshape(-1, LANES),
            custkey.reshape(-1, LANES),
            quarter.reshape(-1, LANES),
            revenue.reshape(-1, LANES),
        )
        cubes = lax.all_to_all(partial_cubes, ("shard", "replica"), 0, 0)
        return jnp.sum(cubes, axis=0)[:SEGMENTS, :QUARTERS]

    return jax.shard_map(
        per_device,
        mesh=mesh,
        in_specs=(
            P(("shard", "replica")),
            P(("shard", "replica")),
            P(("shard", "replica")),
            P("shard"),
            P("shard"),
        ),
        out_specs=P(),
        check_vma=False,
    )
```

```python
import jax
import jax.numpy as jnp
from jax import lax
from jax.experimental import pallas as pl
from jax.experimental.pallas import tpu as pltpu
from jax.sharding import PartitionSpec as P

SEGMENTS = 5
QUARTERS = 28
SUBLANES = 8
LANES = 128
STEP = 8.0
SPAN = 32
PACKED = (4, LANES)
ROWS_AT_ONCE = 64
CHUNKS_AT_ONCE = 8
PARAMS = pltpu.CompilerParams(vmem_limit_bytes=4 * 2**20)


def iota(shape, dim):
    return lax.broadcasted_iota(jnp.int32, shape, dim)


def pick(lines, index):
    if len(lines) == 1:
        return lines[0]
    odd = (index & (len(lines) // 2)) != 0
    half = len(lines) // 2
    return jnp.where(odd, pick(lines[half:], index), pick(lines[:half], index))


def cube_kernel(table_ref, custkey_ref, quarter_ref, revenue_ref, out_ref, segment_ref, w1_ref, w2_ref, w3_ref):
    rows = table_ref.shape[0]
    facts = custkey_ref.shape[0]
    tile = (SUBLANES, LANES)
    zero = jnp.zeros(tile, jnp.float32)

    def look(at):
        key = custkey_ref[at, :]
        high = key >> 7
        low = key & (LANES - 1)

        def block(b, found):
            base = pl.multiple_of(b * ROWS_AT_ONCE, ROWS_AT_ONCE)
            lines = [
                jnp.take_along_axis(jnp.broadcast_to(table_ref[pl.ds(base + r, 1), :], tile), low, axis=1)
                for r in range(ROWS_AT_ONCE)
            ]
            return jnp.where((high // ROWS_AT_ONCE) == b, pick(lines, high), found)

        if rows == ROWS_AT_ONCE:
            return block(0, zero)
        return lax.fori_loop(0, rows // ROWS_AT_ONCE, block, zero)

    def add(chunk, total):
        base = pl.multiple_of(chunk * SUBLANES, SUBLANES)
        at = pl.ds(base, SUBLANES)
        found = look(at)
        segment = jnp.floor(found * (1.0 / STEP))
        weight = revenue_ref[at, :] * (found - segment * STEP)
        w1 = weight.astype(jnp.bfloat16).astype(jnp.float32)
        rest = weight - w1
        w2 = rest.astype(jnp.bfloat16).astype(jnp.float32)
        segment_ref[at, :] = segment.astype(jnp.int32)
        w1_ref[at, :] = w1
        w2_ref[at, :] = w2
        w3_ref[at, :] = rest - w2
        left, right = [], []
        for r in range(SUBLANES):
            row = pl.ds(base + r, 1)
            mine = jnp.broadcast_to(segment_ref[row, :], tile) == iota(tile, 0)
            parts = [jnp.where(mine, jnp.broadcast_to(w[row, :], tile), 0.0) for w in (w1_ref, w2_ref, w3_ref)]
            left.append(jnp.concatenate([*parts, zero], axis=0).astype(jnp.bfloat16))
            wide = (SPAN, LANES)
            hit = jnp.broadcast_to(quarter_ref[row, :], wide) == iota(wide, 0)
            right.append(jnp.where(hit, 1.0, 0.0).astype(jnp.bfloat16))
        return total + lax.dot_general(
            jnp.concatenate(left, axis=1),
            jnp.concatenate(right, axis=1),
            (((1,), (1,)), ((), ())),
            preferred_element_type=jnp.float32,
        )

    def several(step, total):
        for c in range(CHUNKS_AT_ONCE):
            total = add(step * CHUNKS_AT_ONCE + c, total)
        return total

    total = jnp.zeros((4 * SUBLANES, SPAN), jnp.float32)
    steps = facts // (SUBLANES * CHUNKS_AT_ONCE)
    total = several(0, total) if steps == 1 else lax.fori_loop(0, steps, several, total)
    cube = total[0:8] + total[8:16] + total[16:24]
    cube = jnp.concatenate([cube, jnp.zeros((SUBLANES, LANES - SPAN), jnp.float32)], axis=1)
    packed = (cube + pltpu.roll(pltpu.roll(cube, SPAN, 1), SUBLANES - PACKED[0], 0))[: PACKED[0]]
    for d in range(out_ref.shape[0]):
        out_ref[d] = packed


def sum_kernel(cubes_ref, out_ref):
    total = cubes_ref[0]
    for d in range(1, cubes_ref.shape[0]):
        total = total + cubes_ref[d]
    out_ref[: PACKED[0], :] = total[:, :QUARTERS]
    out_ref[PACKED[0] :, :] = total[: SEGMENTS - PACKED[0], SPAN : SPAN + QUARTERS]


def solution(mesh):
    shards = mesh.shape["shard"]
    everyone = shards * mesh.shape["replica"]

    def per_device(custkey, quarter, revenue, segment, rate):
        mine = segment.astype(jnp.float32) * STEP + rate.astype(jnp.float32)
        mine = mine.reshape(-1, LANES)
        table = lax.all_to_all(
            jnp.broadcast_to(mine[None], (shards, *mine.shape)), "shard", 0, 0
        )
        facts = custkey.reshape(-1, LANES).shape
        partial_cubes = pl.pallas_call(
            cube_kernel,
            out_shape=jax.ShapeDtypeStruct((everyone, *PACKED), jnp.float32),
            scratch_shapes=[pltpu.VMEM(facts, jnp.int32)] + [pltpu.VMEM(facts, jnp.float32)] * 3,
            compiler_params=PARAMS,
        )(
            table.reshape(-1, LANES),
            custkey.reshape(facts),
            quarter.reshape(facts),
            revenue.reshape(facts),
        )
        cubes = lax.all_to_all(partial_cubes, ("shard", "replica"), 0, 0)
        return pl.pallas_call(
            sum_kernel,
            out_shape=jax.ShapeDtypeStruct((SEGMENTS, QUARTERS), jnp.float32),
            compiler_params=PARAMS,
        )(cubes)

    return jax.shard_map(
        per_device,
        mesh=mesh,
        in_specs=(
            P(("shard", "replica")),
            P(("shard", "replica")),
            P(("shard", "replica")),
            P("shard"),
            P("shard"),
        ),
        out_specs=P(),
        check_vma=False,
    )
```

```python
import functools

import jax
import jax.numpy as jnp
from jax import lax
from jax.experimental import pallas as pl
from jax.experimental.pallas import tpu as pltpu
from jax.sharding import PartitionSpec as P

SEGMENTS = 5
QUARTERS = 28
SUBLANES = 8
LANES = 128
STEP = 8.0
UNIT = 512.0
SEGMENT_BITS = 12
SPAN = 32
PACKED = (4, LANES)
WORDS_AT_ONCE = 32
CHUNKS_AT_ONCE = 8
PARAMS = pltpu.CompilerParams(vmem_limit_bytes=4 * 2**20)


def iota(shape, dim):
    return lax.broadcasted_iota(jnp.int32, shape, dim)


def pick(lines, index):
    if len(lines) == 1:
        return lines[0]
    odd = (index & (len(lines) // 2)) != 0
    half = len(lines) // 2
    return jnp.where(odd, pick(lines[half:], index), pick(lines[:half], index))


def cube_kernel(order, table_ref, custkey_ref, quarter_ref, revenue_ref, out_ref, word_ref, segment_ref, w1_ref, w2_ref, w3_ref):
    facts = custkey_ref.shape[0]
    words = word_ref.shape[0]
    part = 2 * words // len(order)
    tile = (SUBLANES, LANES)
    zero = jnp.zeros(tile, jnp.float32)

    def code(row):
        slot = order.index(row // part)
        return (table_ref[pl.ds(slot * part + row % part, SUBLANES), :] * UNIT).astype(jnp.int32)

    for row in range(0, words, SUBLANES):
        word_ref[pl.ds(row, SUBLANES), :] = code(row) | (code(row + words) << 16)

    def look(at):
        key = custkey_ref[at, :]
        low = key & (LANES - 1)
        high = key >> 7
        second = high >= words
        high = jnp.where(second, high - words, high)

        def block(b, found):
            base = pl.multiple_of(b * WORDS_AT_ONCE, WORDS_AT_ONCE)
            lines = [
                jnp.take_along_axis(jnp.broadcast_to(word_ref[pl.ds(base + r, 1), :], tile), low, axis=1)
                for r in range(WORDS_AT_ONCE)
            ]
            got = pick(lines, high)
            return got if found is None else jnp.where(high // WORDS_AT_ONCE == b, got, found)

        if words == WORDS_AT_ONCE:
            word = block(0, None)
        else:
            word = lax.fori_loop(0, words // WORDS_AT_ONCE, block, jnp.zeros(tile, jnp.int32))
        return jnp.where(second, word >> 16, word & 0xFFFF)

    def add(chunk, total):
        base = pl.multiple_of(chunk * SUBLANES, SUBLANES)
        at = pl.ds(base, SUBLANES)
        found = look(at)
        rate = (found & ((1 << SEGMENT_BITS) - 1)).astype(jnp.float32) * (1.0 / UNIT)
        weight = revenue_ref[at, :] * rate
        w1 = weight.astype(jnp.bfloat16).astype(jnp.float32)
        rest = weight - w1
        w2 = rest.astype(jnp.bfloat16).astype(jnp.float32)
        segment_ref[at, :] = found >> SEGMENT_BITS
        w1_ref[at, :] = w1
        w2_ref[at, :] = w2
        w3_ref[at, :] = rest - w2
        left, right = [], []
        for r in range(SUBLANES):
            row = pl.ds(base + r, 1)
            mine = jnp.broadcast_to(segment_ref[row, :], tile) == iota(tile, 0)
            parts = [jnp.where(mine, jnp.broadcast_to(w[row, :], tile), 0.0) for w in (w1_ref, w2_ref, w3_ref)]
            left.append(jnp.concatenate([*parts, zero], axis=0).astype(jnp.bfloat16))
            wide = (SPAN, LANES)
            hit = jnp.broadcast_to(quarter_ref[row, :], wide) == iota(wide, 0)
            right.append(jnp.where(hit, 1.0, 0.0).astype(jnp.bfloat16))
        return total + lax.dot_general(
            jnp.concatenate(left, axis=1),
            jnp.concatenate(right, axis=1),
            (((1,), (1,)), ((), ())),
            preferred_element_type=jnp.float32,
        )

    def several(step, total):
        for c in range(CHUNKS_AT_ONCE):
            total = add(step * CHUNKS_AT_ONCE + c, total)
        return total

    total = jnp.zeros((4 * SUBLANES, SPAN), jnp.float32)
    steps = facts // (SUBLANES * CHUNKS_AT_ONCE)
    total = several(0, total) if steps == 1 else lax.fori_loop(0, steps, several, total)
    cube = total[0:8] + total[8:16] + total[16:24]
    cube = jnp.concatenate([cube, jnp.zeros((SUBLANES, LANES - SPAN), jnp.float32)], axis=1)
    out_ref[...] = (cube + pltpu.roll(pltpu.roll(cube, SPAN, 1), SUBLANES - PACKED[0], 0))[: PACKED[0]]


def sum_kernel(cubes_ref, out_ref):
    total = cubes_ref[0]
    for d in range(1, cubes_ref.shape[0]):
        total = total + cubes_ref[d]
    out_ref[: PACKED[0], :] = total[:, :QUARTERS]
    out_ref[PACKED[0] :, :] = total[: SEGMENTS - PACKED[0], SPAN : SPAN + QUARTERS]


def solution(mesh):
    shards, replicas = mesh.shape["shard"], mesh.shape["replica"]
    middle = shards // 2 + 1
    order = [middle] + [s for s in range(shards) if s != middle]
    pairs = [(s, r) for s in range(0, shards, 2) for r in range(replicas)]
    pairs = [pairs[-1]] + pairs[:-1]
    halves = [[(s + (half if s + r else 1 - half)) * replicas + r for s, r in pairs] for half in (1, 0)]

    def per_device(custkey, quarter, revenue, segment, rate):
        mine = segment.astype(jnp.float32) * STEP + rate.astype(jnp.float32)
        mine = mine.reshape(-1, LANES)
        table = lax.all_to_all(
            jnp.broadcast_to(mine[None], (shards, *mine.shape)), "shard", 0, 0, axis_index_groups=[order]
        )
        table = table.reshape(-1, LANES)
        facts = custkey.reshape(-1, LANES).shape
        cube = pl.pallas_call(
            functools.partial(cube_kernel, order),
            out_shape=jax.ShapeDtypeStruct(PACKED, jnp.float32),
            scratch_shapes=[
                pltpu.VMEM((table.shape[0] // 2, LANES), jnp.int32),
                pltpu.VMEM(facts, jnp.int32),
                *[pltpu.VMEM(facts, jnp.float32)] * 3,
            ],
            compiler_params=PARAMS,
        )(table, custkey.reshape(facts), quarter.reshape(facts), revenue.reshape(facts))
        cube = cube + lax.ppermute(cube, "shard", [(s, s ^ 1) for s in range(shards)])
        cubes = lax.all_to_all(
            jnp.broadcast_to(cube[None], (len(pairs), *PACKED)), ("shard", "replica"), 0, 0, axis_index_groups=halves
        )
        return pl.pallas_call(
            sum_kernel,
            out_shape=jax.ShapeDtypeStruct((SEGMENTS, QUARTERS), jnp.float32),
            compiler_params=PARAMS,
        )(cubes)

    return jax.shard_map(
        per_device,
        mesh=mesh,
        in_specs=(
            P(("shard", "replica")),
            P(("shard", "replica")),
            P(("shard", "replica")),
            P("shard"),
            P("shard"),
        ),
        out_specs=P(),
        check_vma=False,
    )
```

```python
import functools

import jax
import jax.numpy as jnp
from jax import lax
from jax.experimental import pallas as pl
from jax.experimental.pallas import tpu as pltpu
from jax.sharding import PartitionSpec as P

SEGMENTS = 5
QUARTERS = 28
SUBLANES = 8
LANES = 128
STEP = 8.0
UNIT = 512.0
SEGMENT_BITS = 12
SPAN = 32
PACKED = (4, LANES)
WORDS_AT_ONCE = 32
CHUNKS_AT_ONCE = 8
PARAMS = pltpu.CompilerParams(vmem_limit_bytes=4 * 2**20)


def iota(shape, dim):
    return lax.broadcasted_iota(jnp.int32, shape, dim)


def pack_kernel(segment_ref, rate_ref, out_ref):
    mine = segment_ref[...].astype(jnp.float32) * STEP + rate_ref[...].astype(jnp.float32)
    for s in range(out_ref.shape[0]):
        out_ref[s] = mine


def pick(lines, index):
    if len(lines) == 1:
        return lines[0]
    odd = (index & (len(lines) // 2)) != 0
    half = len(lines) // 2
    return jnp.where(odd, pick(lines[half:], index), pick(lines[:half], index))


def cube_kernel(order, table_ref, *refs):
    sources, (out_ref, word_ref, segment_ref, w1_ref, w2_ref, w3_ref) = (refs[0:3], refs[3:6]), refs[6:]
    facts = sources[0][0].shape[0]
    words = word_ref.shape[0]
    part = 2 * words // len(order)
    tile = (SUBLANES, LANES)
    zero = jnp.zeros(tile, jnp.float32)

    def code(row):
        slot = order.index(row // part)
        return (table_ref[pl.ds(slot * part + row % part, SUBLANES), :] * UNIT).astype(jnp.int32)

    for row in range(0, words, SUBLANES):
        word_ref[pl.ds(row, SUBLANES), :] = code(row) | (code(row + words) << 16)

    def look(key):
        low = key & (LANES - 1)
        high = key >> 7
        second = high >= words
        high = jnp.where(second, high - words, high)

        def block(b, found):
            base = pl.multiple_of(b * WORDS_AT_ONCE, WORDS_AT_ONCE)
            lines = [
                jnp.take_along_axis(jnp.broadcast_to(word_ref[pl.ds(base + r, 1), :], tile), low, axis=1)
                for r in range(WORDS_AT_ONCE)
            ]
            got = pick(lines, high)
            return got if found is None else jnp.where(high // WORDS_AT_ONCE == b, got, found)

        if words == WORDS_AT_ONCE:
            word = block(0, None)
        else:
            word = lax.fori_loop(0, words // WORDS_AT_ONCE, block, jnp.zeros(tile, jnp.int32))
        return jnp.where(second, word >> 16, word & 0xFFFF)

    def add(source, chunk, total):
        custkey_ref, quarter_ref, revenue_ref = sources[source]
        base = pl.multiple_of(chunk * SUBLANES, SUBLANES)
        start = pl.multiple_of(source * facts + base, SUBLANES)
        found = look(custkey_ref[pl.ds(base, SUBLANES), :])
        rate = (found & ((1 << SEGMENT_BITS) - 1)).astype(jnp.float32) * (1.0 / UNIT)
        weight = revenue_ref[pl.ds(base, SUBLANES), :] * rate
        w1 = weight.astype(jnp.bfloat16).astype(jnp.float32)
        rest = weight - w1
        w2 = rest.astype(jnp.bfloat16).astype(jnp.float32)
        at = pl.ds(start, SUBLANES)
        segment_ref[at, :] = found >> SEGMENT_BITS
        w1_ref[at, :] = w1
        w2_ref[at, :] = w2
        w3_ref[at, :] = rest - w2
        left, right = [], []
        for r in range(SUBLANES):
            row = pl.ds(start + r, 1)
            mine = jnp.broadcast_to(segment_ref[row, :], tile) == iota(tile, 0)
            parts = [jnp.where(mine, jnp.broadcast_to(w[row, :], tile), 0.0) for w in (w1_ref, w2_ref, w3_ref)]
            left.append(jnp.concatenate([*parts, zero], axis=0).astype(jnp.bfloat16))
            wide = (SPAN, LANES)
            hit = jnp.broadcast_to(quarter_ref[pl.ds(base + r, 1), :], wide) == iota(wide, 0)
            right.append(jnp.where(hit, 1.0, 0.0).astype(jnp.bfloat16))
        return total + lax.dot_general(
            jnp.concatenate(left, axis=1),
            jnp.concatenate(right, axis=1),
            (((1,), (1,)), ((), ())),
            preferred_element_type=jnp.float32,
        )

    def several(step, totals):
        for c in range(CHUNKS_AT_ONCE):
            totals = tuple(add(i, step * CHUNKS_AT_ONCE + c, total) for i, total in enumerate(totals))
        return totals

    totals = (jnp.zeros((4 * SUBLANES, SPAN), jnp.float32),) * len(sources)
    steps = facts // (SUBLANES * CHUNKS_AT_ONCE)
    totals = several(0, totals) if steps == 1 else lax.fori_loop(0, steps, several, totals)
    total = totals[0] + totals[1]
    cube = total[0:8] + total[8:16] + total[16:24]
    cube = jnp.concatenate([cube, jnp.zeros((SUBLANES, LANES - SPAN), jnp.float32)], axis=1)
    packed = (cube + pltpu.roll(pltpu.roll(cube, SPAN, 1), SUBLANES - PACKED[0], 0))[: PACKED[0]]
    for d in range(out_ref.shape[0]):
        out_ref[d] = packed


def sum_kernel(cubes_ref, out_ref):
    total = cubes_ref[0]
    for d in range(1, cubes_ref.shape[0]):
        total = total + cubes_ref[d]
    out_ref[: PACKED[0], :] = total[:, :QUARTERS]
    out_ref[PACKED[0] :, :] = total[: SEGMENTS - PACKED[0], SPAN : SPAN + QUARTERS]


def solution(mesh):
    shards, replicas = mesh.shape["shard"], mesh.shape["replica"]
    middle = shards // 2 + 1
    order = [middle] + [s for s in range(shards) if s != middle]
    pairs = [(s, r) for s in range(0, shards, 2) for r in range(replicas)]
    pairs = [pairs[-1]] + pairs[:-1]
    halves = [[(s + (half if s + r else 1 - half)) * replicas + r for s, r in pairs] for half in (1, 0)]

    def per_device(custkey, quarter, revenue, segment, rate):
        facts = custkey.reshape(-1, LANES).shape
        own = [a.reshape(facts) for a in (custkey, quarter, revenue)]
        partner = [lax.ppermute(a, "shard", [(s, s ^ 1) for s in range(shards)]) for a in own]
        block = (segment.shape[0] // LANES, LANES)
        mine = pl.pallas_call(
            pack_kernel,
            out_shape=jax.ShapeDtypeStruct((shards, *block), jnp.float32),
            compiler_params=PARAMS,
        )(segment.reshape(block), rate.reshape(block))
        table = lax.all_to_all(mine, "shard", 0, 0, axis_index_groups=[order])
        table = table.reshape(-1, LANES)
        both = (2 * facts[0], LANES)
        cubes = pl.pallas_call(
            functools.partial(cube_kernel, order),
            out_shape=jax.ShapeDtypeStruct((len(pairs), *PACKED), jnp.float32),
            scratch_shapes=[
                pltpu.VMEM((table.shape[0] // 2, LANES), jnp.int32),
                pltpu.VMEM(both, jnp.int32),
                *[pltpu.VMEM(both, jnp.float32)] * 3,
            ],
            compiler_params=PARAMS,
        )(table, *own, *partner)
        cubes = lax.all_to_all(cubes, ("shard", "replica"), 0, 0, axis_index_groups=halves)
        return pl.pallas_call(
            sum_kernel,
            out_shape=jax.ShapeDtypeStruct((SEGMENTS, QUARTERS), jnp.float32),
            compiler_params=PARAMS,
        )(cubes)

    return jax.shard_map(
        per_device,
        mesh=mesh,
        in_specs=(
            P(("shard", "replica")),
            P(("shard", "replica")),
            P(("shard", "replica")),
            P("shard"),
            P("shard"),
        ),
        out_specs=P(),
        check_vma=False,
    )
```

```python
import functools

import jax
import jax.numpy as jnp
from jax import lax
from jax.experimental import pallas as pl
from jax.experimental.pallas import tpu as pltpu
from jax.sharding import PartitionSpec as P

SEGMENTS = 5
QUARTERS = 28
SUBLANES = 8
LANES = 128
STEP = 8.0
UNIT = 512.0
SEGMENT_BITS = 12
SPAN = 32
PACKED = (4, LANES)
WORDS_AT_ONCE = 32
CHUNKS_AT_ONCE = 8
PARAMS = pltpu.CompilerParams(vmem_limit_bytes=4 * 2**20)


def iota(shape, dim):
    return lax.broadcasted_iota(jnp.int32, shape, dim)


def pick(lines, index):
    if len(lines) == 1:
        return lines[0]
    odd = (index & (len(lines) // 2)) != 0
    half = len(lines) // 2
    return jnp.where(odd, pick(lines[half:], index), pick(lines[:half], index))


def cube_kernel(offsets, *refs):
    tables, refs = refs[: len(offsets)], refs[len(offsets) :]
    sources, (out_ref, code_ref, word_ref, quarter_ref, segment_ref, w1_ref, w2_ref, w3_ref) = (refs[0:3], refs[3:6]), refs[6:]
    facts = segment_ref.shape[0] // len(sources)
    words = word_ref.shape[0]
    tile = (SUBLANES, LANES)
    zero = jnp.zeros(tile, jnp.float32)

    me = lax.axis_index("shard")
    for offset, table_ref in zip(offsets, tables):
        pair, part, _ = table_ref.shape
        for i in range(pair):
            block = pl.multiple_of((me ^ (offset ^ i)) * part, part)
            code_ref[pl.ds(block, part), :] = (table_ref[i] * UNIT).astype(jnp.int32)
    word_ref[...] = code_ref[pl.ds(0, words), :] | (code_ref[pl.ds(words, words), :] << 16)

    def look(key):
        low = key & (LANES - 1)
        high = key >> 7
        second = high >= words
        high = jnp.where(second, high - words, high)

        def block(b, found):
            base = pl.multiple_of(b * WORDS_AT_ONCE, WORDS_AT_ONCE)
            lines = [
                jnp.take_along_axis(jnp.broadcast_to(word_ref[pl.ds(base + r, 1), :], tile), low, axis=1)
                for r in range(WORDS_AT_ONCE)
            ]
            got = pick(lines, high)
            return got if found is None else jnp.where(high // WORDS_AT_ONCE == b, got, found)

        if words == WORDS_AT_ONCE:
            word = block(0, None)
        else:
            word = lax.fori_loop(0, words // WORDS_AT_ONCE, block, jnp.zeros(tile, jnp.int32))
        return jnp.where(second, word >> 16, word & 0xFFFF)

    def add(source, chunk, total):
        custkey_ref, quarters_ref, revenue_ref = sources[source]
        base = pl.multiple_of(chunk * SUBLANES, SUBLANES)
        start = pl.multiple_of(source * facts + base, SUBLANES)
        found = look(custkey_ref[pl.ds(base, SUBLANES), :].astype(jnp.int32))
        rate = (found & ((1 << SEGMENT_BITS) - 1)).astype(jnp.float32) * (1.0 / UNIT)
        weight = revenue_ref[pl.ds(base, SUBLANES), :] * rate
        w1 = weight.astype(jnp.bfloat16).astype(jnp.float32)
        rest = weight - w1
        w2 = rest.astype(jnp.bfloat16).astype(jnp.float32)
        at = pl.ds(start, SUBLANES)
        segment_ref[at, :] = found >> SEGMENT_BITS
        quarter_ref[at, :] = quarters_ref[pl.ds(base, SUBLANES), :].astype(jnp.int32)
        w1_ref[at, :] = w1
        w2_ref[at, :] = w2
        w3_ref[at, :] = rest - w2
        left, right = [], []
        for r in range(SUBLANES):
            row = pl.ds(start + r, 1)
            mine = jnp.broadcast_to(segment_ref[row, :], tile) == iota(tile, 0)
            parts = [jnp.where(mine, jnp.broadcast_to(w[row, :], tile), 0.0) for w in (w1_ref, w2_ref, w3_ref)]
            left.append(jnp.concatenate([*parts, zero], axis=0).astype(jnp.bfloat16))
            wide = (SPAN, LANES)
            hit = jnp.broadcast_to(quarter_ref[row, :], wide) == iota(wide, 0)
            right.append(jnp.where(hit, 1.0, 0.0).astype(jnp.bfloat16))
        return total + lax.dot_general(
            jnp.concatenate(left, axis=1),
            jnp.concatenate(right, axis=1),
            (((1,), (1,)), ((), ())),
            preferred_element_type=jnp.float32,
        )

    def several(step, totals):
        for c in range(CHUNKS_AT_ONCE):
            totals = tuple(add(i, step * CHUNKS_AT_ONCE + c, total) for i, total in enumerate(totals))
        return totals

    totals = (jnp.zeros((4 * SUBLANES, SPAN), jnp.float32),) * len(sources)
    steps = facts // (SUBLANES * CHUNKS_AT_ONCE)
    totals = several(0, totals) if steps == 1 else lax.fori_loop(0, steps, several, totals)
    total = totals[0] + totals[1]
    cube = total[0:8] + total[8:16] + total[16:24]
    cube = jnp.concatenate([cube, jnp.zeros((SUBLANES, LANES - SPAN), jnp.float32)], axis=1)
    packed = (cube + pltpu.roll(pltpu.roll(cube, SPAN, 1), SUBLANES - PACKED[0], 0))[: PACKED[0]]
    for d in range(out_ref.shape[0]):
        out_ref[d] = packed


def sum_kernel(cubes_ref, out_ref):
    total = cubes_ref[0]
    for d in range(1, cubes_ref.shape[0]):
        total = total + cubes_ref[d]
    out_ref[: PACKED[0], :] = total[:, :QUARTERS]
    out_ref[PACKED[0] :, :] = total[: SEGMENTS - PACKED[0], SPAN : SPAN + QUARTERS]


def solution(mesh):
    shards, replicas = mesh.shape["shard"], mesh.shape["replica"]
    offsets = [k + 1 for k in range(2, shards, 2)]
    pairs = [(s, r) for s in range(0, shards, 2) for r in range(replicas)]
    pairs = [pairs[-1]] + pairs[:-1]
    halves = [[(s + (half if s + r else 1 - half)) * replicas + r for s, r in pairs] for half in (1, 0)]

    def per_device(custkey, quarter, revenue, segment, rate):
        def swap(a, offset):
            return lax.ppermute(a, "shard", [(s, s ^ offset) for s in range(shards)])

        block = (segment.shape[0] // LANES, LANES)
        facts = custkey.reshape(-1, LANES).shape
        loaded = [a.reshape(facts) for a in (custkey, quarter, revenue)]
        mine = (segment.astype(jnp.float32) * STEP + rate.astype(jnp.float32)).reshape(1, *block)
        mine, *sent = lax.optimization_barrier((mine, *loaded))
        other = swap(mine, 1)
        partner = [swap(a, 1) for a in sent]
        table = jnp.concatenate([mine, other])
        tables = [table] + [swap(table, k) for k in offsets]
        table, *kept = lax.optimization_barrier((table, *loaded))
        own = [a.astype(jnp.float32) for a in kept]
        both = (2 * facts[0], LANES)
        cubes = pl.pallas_call(
            functools.partial(cube_kernel, [0] + offsets),
            out_shape=jax.ShapeDtypeStruct((len(pairs), *PACKED), jnp.float32),
            scratch_shapes=[
                pltpu.VMEM((shards * block[0], LANES), jnp.int32),
                pltpu.VMEM((shards * block[0] // 2, LANES), jnp.int32),
                *[pltpu.VMEM(both, jnp.int32)] * 2,
                *[pltpu.VMEM(both, jnp.float32)] * 3,
            ],
            compiler_params=PARAMS,
        )(*tables, *own, *partner)
        cubes = lax.all_to_all(cubes, ("shard", "replica"), 0, 0, axis_index_groups=halves)
        return pl.pallas_call(
            sum_kernel,
            out_shape=jax.ShapeDtypeStruct((SEGMENTS, QUARTERS), jnp.float32),
            compiler_params=PARAMS,
        )(cubes)

    return jax.shard_map(
        per_device,
        mesh=mesh,
        in_specs=(
            P(("shard", "replica")),
            P(("shard", "replica")),
            P(("shard", "replica")),
            P("shard"),
            P("shard"),
        ),
        out_specs=P(),
        check_vma=False,
    )
```

```python
import functools

import jax
import jax.numpy as jnp
from jax import lax
from jax.experimental import pallas as pl
from jax.experimental.pallas import tpu as pltpu
from jax.sharding import PartitionSpec as P

SEGMENTS = 5
QUARTERS = 28
SUBLANES = 8
LANES = 128
STEP = 8.0
UNIT = 512.0
SEGMENT_BITS = 12
SPAN = 32
PACKED = (4, LANES)
CHUNKS_AT_ONCE = 8
PARAMS = pltpu.CompilerParams(vmem_limit_bytes=4 * 2**20)


def iota(shape, dim):
    return lax.broadcasted_iota(jnp.int32, shape, dim)


def pick(lines, index):
    if len(lines) == 1:
        return lines[0]
    odd = (index & (len(lines) // 2)) != 0
    half = len(lines) // 2
    return jnp.where(odd, pick(lines[half:], index), pick(lines[:half], index))


def look(offset, table_ref, word_ref, key, word):
    part = table_ref.shape[1]
    bits = (LANES * part).bit_length() - 1
    tile = (SUBLANES, LANES)
    low, line, pair = key & (LANES - 1), (key >> 7) & (part - 1), key >> (bits + 1)
    lines = [
        jnp.take_along_axis(jnp.broadcast_to(word_ref[pl.ds(r, 1), :], tile), low, axis=1) for r in range(part)
    ]
    here = (lax.axis_index("shard") ^ offset) >> 1
    return jnp.where(pair == here, pick(lines, line), word)


def join(offset, table_ref, word_ref):
    codes = [(table_ref[i] * UNIT).astype(jnp.int32) for i in range(2)]
    odd = ((lax.axis_index("shard") ^ offset) & 1) == 1
    first, second = jnp.where(odd, codes[1], codes[0]), jnp.where(odd, codes[0], codes[1])
    word_ref[...] = first | (second << 16)


def look_kernel(offsets, fresh, *refs):
    tables, refs = refs[: len(offsets)], refs[len(offsets) :]
    keys, refs = refs[:2], refs[2:]
    before_ref, (out_ref, word_ref) = (None, refs) if fresh else (refs[0], refs[1:])
    for i, (offset, table_ref) in enumerate(zip(offsets, tables)):
        join(offset, table_ref, word_ref.at[i])
    facts = keys[0].shape[0]
    for c in range(0, facts, SUBLANES):
        for source, key_ref in enumerate(keys):
            key = key_ref[pl.ds(c, SUBLANES), :].astype(jnp.int32)
            at = pl.ds(source * facts + c, SUBLANES)
            word = jnp.zeros(key.shape, jnp.int32) if fresh else before_ref[at, :]
            for i, (offset, table_ref) in enumerate(zip(offsets, tables)):
                word = look(offset, table_ref, word_ref.at[i], key, word)
            out_ref[at, :] = word


def cube_kernel(offset, table_ref, before_ref, *refs):
    sources, (out_ref, word_ref, quarter_ref, segment_ref, w1_ref, w2_ref, w3_ref) = (refs[0:3], refs[3:6]), refs[6:]
    facts = sources[0][0].shape[0]
    tile = (SUBLANES, LANES)
    zero = jnp.zeros(tile, jnp.float32)
    half = (LANES * table_ref.shape[1]).bit_length() - 1
    join(offset, table_ref, word_ref)

    def add(source, chunk, total):
        key_ref, quarters_ref, revenue_ref = sources[source]
        base = pl.multiple_of(chunk * SUBLANES, SUBLANES)
        start = pl.multiple_of(source * facts + base, SUBLANES)
        at = pl.ds(start, SUBLANES)
        key = key_ref[pl.ds(base, SUBLANES), :].astype(jnp.int32)
        word = look(offset, table_ref, word_ref, key, before_ref[at, :])
        found = jnp.where(((key >> half) & 1) == 1, word >> 16, word & 0xFFFF)
        rate = (found & ((1 << SEGMENT_BITS) - 1)).astype(jnp.float32) * (1.0 / UNIT)
        weight = revenue_ref[pl.ds(base, SUBLANES), :] * rate
        w1 = weight.astype(jnp.bfloat16).astype(jnp.float32)
        rest = weight - w1
        w2 = rest.astype(jnp.bfloat16).astype(jnp.float32)
        segment_ref[at, :] = found >> SEGMENT_BITS
        quarter_ref[at, :] = quarters_ref[pl.ds(base, SUBLANES), :].astype(jnp.int32)
        w1_ref[at, :] = w1
        w2_ref[at, :] = w2
        w3_ref[at, :] = rest - w2
        left, right = [], []
        for r in range(SUBLANES):
            row = pl.ds(start + r, 1)
            mine = jnp.broadcast_to(segment_ref[row, :], tile) == iota(tile, 0)
            parts = [jnp.where(mine, jnp.broadcast_to(w[row, :], tile), 0.0) for w in (w1_ref, w2_ref, w3_ref)]
            left.append(jnp.concatenate([*parts, zero], axis=0).astype(jnp.bfloat16))
            wide = (SPAN, LANES)
            hit = jnp.broadcast_to(quarter_ref[row, :], wide) == iota(wide, 0)
            right.append(jnp.where(hit, 1.0, 0.0).astype(jnp.bfloat16))
        return total + lax.dot_general(
            jnp.concatenate(left, axis=1),
            jnp.concatenate(right, axis=1),
            (((1,), (1,)), ((), ())),
            preferred_element_type=jnp.float32,
        )

    def several(step, totals):
        for c in range(CHUNKS_AT_ONCE):
            totals = tuple(add(i, step * CHUNKS_AT_ONCE + c, total) for i, total in enumerate(totals))
        return totals

    totals = (jnp.zeros((4 * SUBLANES, SPAN), jnp.float32),) * len(sources)
    steps = facts // (SUBLANES * CHUNKS_AT_ONCE)
    totals = several(0, totals) if steps == 1 else lax.fori_loop(0, steps, several, totals)
    total = totals[0] + totals[1]
    cube = total[0:8] + total[8:16] + total[16:24]
    cube = jnp.concatenate([cube, jnp.zeros((SUBLANES, LANES - SPAN), jnp.float32)], axis=1)
    packed = (cube + pltpu.roll(pltpu.roll(cube, SPAN, 1), SUBLANES - PACKED[0], 0))[: PACKED[0]]
    for d in range(out_ref.shape[0]):
        out_ref[d] = packed


def sum_kernel(cubes_ref, out_ref):
    total = cubes_ref[0]
    for d in range(1, cubes_ref.shape[0]):
        total = total + cubes_ref[d]
    out_ref[: PACKED[0], :] = total[:, :QUARTERS]
    out_ref[PACKED[0] :, :] = total[: SEGMENTS - PACKED[0], SPAN : SPAN + QUARTERS]


def solution(mesh):
    shards, replicas = mesh.shape["shard"], mesh.shape["replica"]
    offsets = [k + 1 for k in range(2, shards, 2)]
    pairs = [(s, r) for s in range(0, shards, 2) for r in range(replicas)]
    pairs = [pairs[-1]] + pairs[:-1]
    halves = [[(s + (half if s + r else 1 - half)) * replicas + r for s, r in pairs] for half in (1, 0)]

    def per_device(custkey, quarter, revenue, segment, rate):
        def swap(a, offset):
            return lax.ppermute(a, "shard", [(s, s ^ offset) for s in range(shards)])

        block = (segment.shape[0] // LANES, LANES)
        facts = custkey.reshape(-1, LANES).shape
        loaded = [a.reshape(facts) for a in (custkey, quarter, revenue)]
        mine = (segment.astype(jnp.float32) * STEP + rate.astype(jnp.float32)).reshape(1, *block)
        mine, *sent = lax.optimization_barrier((mine, *loaded))
        other = swap(mine, 1)
        partner = [swap(a, 1) for a in sent]
        table = jnp.concatenate([mine, other])
        tables = [table] + [swap(table, k) for k in offsets]
        table, *kept = lax.optimization_barrier((table, *loaded))
        own = [a.astype(jnp.float32) for a in kept]
        both = (2 * facts[0], LANES)

        def found(tables, offsets, *before):
            return pl.pallas_call(
                functools.partial(look_kernel, offsets, not before),
                out_shape=jax.ShapeDtypeStruct(both, jnp.int32),
                scratch_shapes=[pltpu.VMEM((len(tables), *block), jnp.int32)],
                compiler_params=PARAMS,
            )(*tables, own[0], partner[0], *before)

        words = found(tables[:1], [0])
        words = found(tables[2:], offsets[1:], words)
        cubes = pl.pallas_call(
            functools.partial(cube_kernel, offsets[0]),
            out_shape=jax.ShapeDtypeStruct((len(pairs), *PACKED), jnp.float32),
            scratch_shapes=[
                pltpu.VMEM(block, jnp.int32),
                *[pltpu.VMEM(both, jnp.int32)] * 2,
                *[pltpu.VMEM(both, jnp.float32)] * 3,
            ],
            compiler_params=PARAMS,
        )(tables[1], words, *own, *partner)
        cubes = lax.all_to_all(cubes, ("shard", "replica"), 0, 0, axis_index_groups=halves)
        return pl.pallas_call(
            sum_kernel,
            out_shape=jax.ShapeDtypeStruct((SEGMENTS, QUARTERS), jnp.float32),
            compiler_params=PARAMS,
        )(cubes)

    return jax.shard_map(
        per_device,
        mesh=mesh,
        in_specs=(
            P(("shard", "replica")),
            P(("shard", "replica")),
            P(("shard", "replica")),
            P("shard"),
            P("shard"),
        ),
        out_specs=P(),
        check_vma=False,
    )
```

```python
import functools

import jax
import jax.numpy as jnp
from jax import lax
from jax.experimental import pallas as pl
from jax.experimental.pallas import tpu as pltpu
from jax.sharding import PartitionSpec as P

SEGMENTS = 5
QUARTERS = 28
SUBLANES = 8
LANES = 128
STEP = 8.0
UNIT = 512.0
SEGMENT_BITS = 12
SPAN = 32
PACKED = (2, LANES)
CHUNKS_AT_ONCE = 8
PARAMS = pltpu.CompilerParams(vmem_limit_bytes=4 * 2**20)


def iota(shape, dim):
    return lax.broadcasted_iota(jnp.int32, shape, dim)


def pick(lines, index):
    if len(lines) == 1:
        return lines[0]
    odd = (index & (len(lines) // 2)) != 0
    half = len(lines) // 2
    return jnp.where(odd, pick(lines[half:], index), pick(lines[:half], index))


def look(offset, table_ref, word_ref, key, word):
    part = table_ref.shape[1]
    bits = (LANES * part).bit_length() - 1
    tile = (SUBLANES, LANES)
    low, line, pair = key & (LANES - 1), (key >> 7) & (part - 1), key >> (bits + 1)
    lines = [
        jnp.take_along_axis(jnp.broadcast_to(word_ref[pl.ds(r, 1), :], tile), low, axis=1) for r in range(part)
    ]
    here = (lax.axis_index("shard") ^ offset) >> 1
    return jnp.where(pair == here, pick(lines, line), word)


def join(offset, table_ref, word_ref):
    codes = [(table_ref[i] * UNIT).astype(jnp.int32) for i in range(2)]
    odd = ((lax.axis_index("shard") ^ offset) & 1) == 1
    first, second = jnp.where(odd, codes[1], codes[0]), jnp.where(odd, codes[0], codes[1])
    word_ref[...] = first | (second << 16)


def look_kernel(offsets, fresh, *refs):
    tables, refs = refs[: len(offsets)], refs[len(offsets) :]
    keys, refs = refs[:2], refs[2:]
    before_ref, (out_ref, word_ref) = (None, refs) if fresh else (refs[0], refs[1:])
    for i, (offset, table_ref) in enumerate(zip(offsets, tables)):
        join(offset, table_ref, word_ref.at[i])
    facts = keys[0].shape[0]
    for c in range(0, facts, SUBLANES):
        for source, key_ref in enumerate(keys):
            key = key_ref[pl.ds(c, SUBLANES), :].astype(jnp.int32)
            at = pl.ds(source * facts + c, SUBLANES)
            word = jnp.zeros(key.shape, jnp.int32) if fresh else before_ref[at, :]
            for i, (offset, table_ref) in enumerate(zip(offsets, tables)):
                word = look(offset, table_ref, word_ref.at[i], key, word)
            out_ref[at, :] = word


def cube_kernel(offset, table_ref, before_ref, *refs):
    sources, (out_ref, word_ref, quarter_ref, segment_ref, w1_ref, w2_ref, w3_ref) = (refs[0:3], refs[3:6]), refs[6:]
    facts = sources[0][0].shape[0]
    tile = (SUBLANES, LANES)
    zero = jnp.zeros(tile, jnp.float32)
    half = (LANES * table_ref.shape[1]).bit_length() - 1
    join(offset, table_ref, word_ref)

    def add(source, chunk, total):
        key_ref, quarters_ref, revenue_ref = sources[source]
        base = pl.multiple_of(chunk * SUBLANES, SUBLANES)
        start = pl.multiple_of(source * facts + base, SUBLANES)
        at = pl.ds(start, SUBLANES)
        key = key_ref[pl.ds(base, SUBLANES), :].astype(jnp.int32)
        word = look(offset, table_ref, word_ref, key, before_ref[at, :])
        found = jnp.where(((key >> half) & 1) == 1, word >> 16, word & 0xFFFF)
        rate = (found & ((1 << SEGMENT_BITS) - 1)).astype(jnp.float32) * (1.0 / UNIT)
        weight = revenue_ref[pl.ds(base, SUBLANES), :] * rate
        w1 = weight.astype(jnp.bfloat16).astype(jnp.float32)
        rest = weight - w1
        w2 = rest.astype(jnp.bfloat16).astype(jnp.float32)
        segment_ref[at, :] = found >> SEGMENT_BITS
        quarter_ref[at, :] = quarters_ref[pl.ds(base, SUBLANES), :].astype(jnp.int32)
        w1_ref[at, :] = w1
        w2_ref[at, :] = w2
        w3_ref[at, :] = rest - w2
        left, right = [], []
        for r in range(SUBLANES):
            row = pl.ds(start + r, 1)
            mine = jnp.broadcast_to(segment_ref[row, :], tile) == iota(tile, 0)
            parts = [jnp.where(mine, jnp.broadcast_to(w[row, :], tile), 0.0) for w in (w1_ref, w2_ref, w3_ref)]
            left.append(jnp.concatenate([*parts, zero], axis=0).astype(jnp.bfloat16))
            wide = (SPAN, LANES)
            hit = jnp.broadcast_to(quarter_ref[row, :], wide) == iota(wide, 0)
            right.append(jnp.where(hit, 1.0, 0.0).astype(jnp.bfloat16))
        return total + lax.dot_general(
            jnp.concatenate(left, axis=1),
            jnp.concatenate(right, axis=1),
            (((1,), (1,)), ((), ())),
            preferred_element_type=jnp.float32,
        )

    def several(step, totals):
        for c in range(CHUNKS_AT_ONCE):
            totals = tuple(add(i, step * CHUNKS_AT_ONCE + c, total) for i, total in enumerate(totals))
        return totals

    totals = (jnp.zeros((4 * SUBLANES, SPAN), jnp.float32),) * len(sources)
    steps = facts // (SUBLANES * CHUNKS_AT_ONCE)
    totals = several(0, totals) if steps == 1 else lax.fori_loop(0, steps, several, totals)
    total = totals[0] + totals[1]
    cube = total[0:8] + total[8:16] + total[16:24]
    cube = jnp.concatenate([cube, jnp.zeros((SUBLANES, LANES - SPAN), jnp.float32)], axis=1)
    row = iota(tile, 0)
    moved = cube
    for s in range(1, LANES // SPAN):
        moved = jnp.where(row == s, pltpu.roll(cube, SPAN * s, 1), moved)
    moved = moved + pltpu.roll(moved, SUBLANES - 1, 0)
    moved = moved + pltpu.roll(moved, SUBLANES - 2, 0)
    packed = jnp.where(row == 1, pltpu.roll(moved, SUBLANES - 3, 0), moved)[: PACKED[0]]
    for d in range(out_ref.shape[0]):
        out_ref[d] = packed


def sum_kernel(cubes_ref, out_ref):
    total = cubes_ref[0]
    for d in range(1, cubes_ref.shape[0]):
        total = total + cubes_ref[d]
    each = LANES // SPAN
    for s in range(SEGMENTS):
        lane = SPAN * (s % each)
        out_ref[s : s + 1, :] = total[s // each : s // each + 1, lane : lane + QUARTERS]


def solution(mesh):
    shards, replicas = mesh.shape["shard"], mesh.shape["replica"]
    offsets = [k + 1 for k in range(2, shards, 2)]
    pairs = [(s, r) for s in range(0, shards, 2) for r in range(replicas)]
    pairs = [pairs[-1]] + pairs[:-1]
    halves = [[(s + (half if s + r else 1 - half)) * replicas + r for s, r in pairs] for half in (1, 0)]

    def per_device(custkey, quarter, revenue, segment, rate):
        def swap(a, offset):
            return lax.ppermute(a, "shard", [(s, s ^ offset) for s in range(shards)])

        block = (segment.shape[0] // LANES, LANES)
        facts = custkey.reshape(-1, LANES).shape
        loaded = [a.reshape(facts) for a in (custkey, quarter, revenue)]
        mine = (segment.astype(jnp.float32) * STEP + rate.astype(jnp.float32)).reshape(1, *block)
        mine, *sent = lax.optimization_barrier((mine, *loaded))
        other = swap(mine, 1)
        partner = [swap(a, 1) for a in sent]
        table = jnp.concatenate([mine, other])
        tables = [table] + [swap(table, k) for k in offsets]
        table, *kept = lax.optimization_barrier((table, *loaded))
        own = [a.astype(jnp.float32) for a in kept]
        both = (2 * facts[0], LANES)

        def found(tables, offsets, *before):
            return pl.pallas_call(
                functools.partial(look_kernel, offsets, not before),
                out_shape=jax.ShapeDtypeStruct(both, jnp.int32),
                scratch_shapes=[pltpu.VMEM((len(tables), *block), jnp.int32)],
                compiler_params=PARAMS,
            )(*tables, own[0], partner[0], *before)

        words = found(tables[:1], [0])
        words = found(tables[2:], offsets[1:], words)
        cubes = pl.pallas_call(
            functools.partial(cube_kernel, offsets[0]),
            out_shape=jax.ShapeDtypeStruct((len(pairs), *PACKED), jnp.float32),
            scratch_shapes=[
                pltpu.VMEM(block, jnp.int32),
                *[pltpu.VMEM(both, jnp.int32)] * 2,
                *[pltpu.VMEM(both, jnp.float32)] * 3,
            ],
            compiler_params=pltpu.CompilerParams(
                vmem_limit_bytes=4 * 2**20
            ),
        )(tables[1], words, *own, *partner)
        cubes = lax.all_to_all(cubes, ("shard", "replica"), 0, 0, axis_index_groups=halves)
        return pl.pallas_call(
            sum_kernel,
            out_shape=jax.ShapeDtypeStruct((SEGMENTS, QUARTERS), jnp.float32),
            compiler_params=PARAMS,
        )(cubes)

    return jax.shard_map(
        per_device,
        mesh=mesh,
        in_specs=(
            P(("shard", "replica")),
            P(("shard", "replica")),
            P(("shard", "replica")),
            P("shard"),
            P("shard"),
        ),
        out_specs=P(),
        check_vma=False,
    )
```

```python
import functools

import jax
import jax.numpy as jnp
from jax import lax
from jax.experimental import pallas as pl
from jax.experimental.pallas import tpu as pltpu
from jax.sharding import PartitionSpec as P

SEGMENTS = 5
QUARTERS = 28
SUBLANES = 8
LANES = 128
STEP = 8.0
UNIT = 512.0
SEGMENT_BITS = 12
SPAN = 32
PACKED = (2, LANES)
CHUNKS_AT_ONCE = 8
PARAMS = pltpu.CompilerParams(vmem_limit_bytes=4 * 2**20)


def iota(shape, dim):
    return lax.broadcasted_iota(jnp.int32, shape, dim)


def pick(lines, index):
    if len(lines) == 1:
        return lines[0]
    odd = (index & (len(lines) // 2)) != 0
    half = len(lines) // 2
    return jnp.where(odd, pick(lines[half:], index), pick(lines[:half], index))


def look(offset, table_ref, word_ref, key, word):
    part = table_ref.shape[1]
    bits = (LANES * part).bit_length() - 1
    tile = (SUBLANES, LANES)
    low, line, pair = key & (LANES - 1), (key >> 7) & (part - 1), key >> (bits + 1)
    lines = [
        jnp.take_along_axis(jnp.broadcast_to(word_ref[pl.ds(r, 1), :], tile), low, axis=1) for r in range(part)
    ]
    here = (lax.axis_index("shard") ^ offset) >> 1
    return jnp.where(pair == here, pick(lines, line), word)


def join(offset, table_ref, word_ref):
    codes = [(table_ref[i] * UNIT).astype(jnp.int32) for i in range(2)]
    odd = ((lax.axis_index("shard") ^ offset) & 1) == 1
    first, second = jnp.where(odd, codes[1], codes[0]), jnp.where(odd, codes[0], codes[1])
    word_ref[...] = first | (second << 16)


def look_kernel(offsets, fresh, *refs):
    tables, refs = refs[: len(offsets)], refs[len(offsets) :]
    keys, refs = refs[:2], refs[2:]
    before_ref, (out_ref, word_ref) = (None, refs) if fresh else (refs[0], refs[1:])
    for i, (offset, table_ref) in enumerate(zip(offsets, tables)):
        join(offset, table_ref, word_ref.at[i])
    facts = keys[0].shape[0]
    for c in range(0, facts, SUBLANES):
        for source, key_ref in enumerate(keys):
            key = key_ref[pl.ds(c, SUBLANES), :].astype(jnp.int32)
            at = pl.ds(source * facts + c, SUBLANES)
            word = jnp.zeros(key.shape, jnp.int32) if fresh else before_ref[at, :]
            for i, (offset, table_ref) in enumerate(zip(offsets, tables)):
                word = look(offset, table_ref, word_ref.at[i], key, word)
            out_ref[at, :] = word


def cube_kernel(offset, table_ref, before_ref, *refs):
    sources, (out_ref, word_ref, quarter_ref, segment_ref, w1_ref, w2_ref, w3_ref) = (refs[0:3], refs[3:6]), refs[6:]
    facts = sources[0][0].shape[0]
    tile = (SUBLANES, LANES)
    zero = jnp.zeros(tile, jnp.float32)
    half = (LANES * table_ref.shape[1]).bit_length() - 1
    join(offset, table_ref, word_ref)

    def add(source, chunk, total):
        key_ref, quarters_ref, revenue_ref = sources[source]
        base = pl.multiple_of(chunk * SUBLANES, SUBLANES)
        start = pl.multiple_of(source * facts + base, SUBLANES)
        at = pl.ds(start, SUBLANES)
        key = key_ref[pl.ds(base, SUBLANES), :].astype(jnp.int32)
        word = look(offset, table_ref, word_ref, key, before_ref[at, :])
        found = jnp.where(((key >> half) & 1) == 1, word >> 16, word & 0xFFFF)
        rate = (found & ((1 << SEGMENT_BITS) - 1)).astype(jnp.float32) * (1.0 / UNIT)
        weight = revenue_ref[pl.ds(base, SUBLANES), :] * rate
        w1 = weight.astype(jnp.bfloat16).astype(jnp.float32)
        rest = weight - w1
        w2 = rest.astype(jnp.bfloat16).astype(jnp.float32)
        segment_ref[at, :] = found >> SEGMENT_BITS
        quarter_ref[at, :] = quarters_ref[pl.ds(base, SUBLANES), :].astype(jnp.int32)
        w1_ref[at, :] = w1
        w2_ref[at, :] = w2
        w3_ref[at, :] = rest - w2
        left, right = [], []
        for r in range(SUBLANES):
            row = pl.ds(start + r, 1)
            mine = jnp.broadcast_to(segment_ref[row, :], tile) == iota(tile, 0)
            parts = [jnp.where(mine, jnp.broadcast_to(w[row, :], tile), 0.0) for w in (w1_ref, w2_ref, w3_ref)]
            left.append(jnp.concatenate([*parts, zero], axis=0).astype(jnp.bfloat16))
            wide = (SPAN, LANES)
            hit = jnp.broadcast_to(quarter_ref[row, :], wide) == iota(wide, 0)
            right.append(jnp.where(hit, 1.0, 0.0).astype(jnp.bfloat16))
        return total + lax.dot_general(
            jnp.concatenate(left, axis=1),
            jnp.concatenate(right, axis=1),
            (((1,), (1,)), ((), ())),
            preferred_element_type=jnp.float32,
        )

    def several(step, totals):
        for c in range(CHUNKS_AT_ONCE):
            totals = tuple(add(i, step * CHUNKS_AT_ONCE + c, total) for i, total in enumerate(totals))
        return totals

    totals = (jnp.zeros((4 * SUBLANES, SPAN), jnp.float32),) * len(sources)
    steps = facts // (SUBLANES * CHUNKS_AT_ONCE)
    totals = several(0, totals) if steps == 1 else lax.fori_loop(0, steps, several, totals)
    total = totals[0] + totals[1]
    cube = total[0:8] + total[8:16] + total[16:24]
    cube = jnp.concatenate([cube, jnp.zeros((SUBLANES, LANES - SPAN), jnp.float32)], axis=1)
    row = iota(tile, 0)
    moved = cube
    for s in range(1, LANES // SPAN):
        moved = jnp.where(row == s, pltpu.roll(cube, SPAN * s, 1), moved)
    moved = moved + pltpu.roll(moved, SUBLANES - 1, 0)
    moved = moved + pltpu.roll(moved, SUBLANES - 2, 0)
    packed = jnp.where(row == 1, pltpu.roll(moved, SUBLANES - 3, 0), moved)[: PACKED[0]]
    for d in range(out_ref.shape[0]):
        out_ref[d] = packed


def sum_kernel(cubes_ref, out_ref):
    parts = [cubes_ref[d] for d in range(cubes_ref.shape[0])]
    while len(parts) > 1:
        parts = [a + b for a, b in zip(parts[::2], parts[1::2])]
    (total,) = parts
    each = LANES // SPAN
    for s in range(SEGMENTS):
        lane = SPAN * (s % each)
        out_ref[s : s + 1, :] = total[s // each : s // each + 1, lane : lane + QUARTERS]


def solution(mesh):
    shards, replicas = mesh.shape["shard"], mesh.shape["replica"]
    offsets = [k + 1 for k in range(2, shards, 2)]
    pairs = [(s, r) for s in range(0, shards, 2) for r in range(replicas)]
    pairs = [pairs[-1]] + pairs[:-1]
    halves = [[(s + (half if s + r else 1 - half)) * replicas + r for s, r in pairs] for half in (1, 0)]

    def per_device(custkey, quarter, revenue, segment, rate):
        def swap(a, offset):
            return lax.ppermute(a, "shard", [(s, s ^ offset) for s in range(shards)])

        block = (segment.shape[0] // LANES, LANES)
        facts = custkey.reshape(-1, LANES).shape
        loaded = [a.reshape(facts) for a in (custkey, quarter, revenue)]
        mine = (segment.astype(jnp.float32) * STEP + rate.astype(jnp.float32)).reshape(1, *block)
        mine, *sent = lax.optimization_barrier((mine, *loaded))
        other = swap(mine, 1)
        partner = [swap(a, 1) for a in sent]
        table = jnp.concatenate([mine, other])
        tables = [table] + [swap(table, k) for k in offsets]
        table, *kept = lax.optimization_barrier((table, *loaded))
        own = [a.astype(jnp.float32) for a in kept]
        both = (2 * facts[0], LANES)

        def found(tables, offsets, *before):
            return pl.pallas_call(
                functools.partial(look_kernel, offsets, not before),
                out_shape=jax.ShapeDtypeStruct(both, jnp.int32),
                scratch_shapes=[pltpu.VMEM((len(tables), *block), jnp.int32)],
                compiler_params=PARAMS,
            )(*tables, own[0], partner[0], *before)

        words = found(tables[:1], [0])
        words = found(tables[2:], offsets[1:], words)
        cubes = pl.pallas_call(
            functools.partial(cube_kernel, offsets[0]),
            out_shape=jax.ShapeDtypeStruct((len(pairs), *PACKED), jnp.float32),
            scratch_shapes=[
                pltpu.VMEM(block, jnp.int32),
                *[pltpu.VMEM(both, jnp.int32)] * 2,
                *[pltpu.VMEM(both, jnp.float32)] * 3,
            ],
            compiler_params=pltpu.CompilerParams(
                vmem_limit_bytes=4 * 2**20
            ),
        )(tables[1], words, *own, *partner)
        cubes = lax.all_to_all(cubes, ("shard", "replica"), 0, 0, axis_index_groups=halves)
        return pl.pallas_call(
            sum_kernel,
            out_shape=jax.ShapeDtypeStruct((SEGMENTS, QUARTERS), jnp.float32),
            compiler_params=PARAMS,
        )(cubes)

    return jax.shard_map(
        per_device,
        mesh=mesh,
        in_specs=(
            P(("shard", "replica")),
            P(("shard", "replica")),
            P(("shard", "replica")),
            P("shard"),
            P("shard"),
        ),
        out_specs=P(),
        check_vma=False,
    )
```
